32 devices in a mesh: gx: 8 (over z, x), gy: 4 (over y, core).
Axes of the slice: x: 2, y: 2, z: 4, core: 2. Of those that a mesh axis runs over, the one named last changes fastest.
Arguments:
- dense_grads: float32 [32, 256, 1024], P(('gx', 'gy')), may hold values from -6 to 6
- dense_param: float32 [256, 1024], P(('gx', 'gy')), may hold values from -6 to 6
- dense_acc: float32 [256, 1024], P(('gx', 'gy'))
- table: float32 [131072, 128], P(('gx', 'gy')), may hold values from -6 to 6
- row_acc: float32 [131072], P(('gx', 'gy'))
- touched: int32 [16384], P(('gx', 'gy')), may hold values from 0 to 4095, as said below
- emb_grads: float32 [16384, 128], P(('gx', 'gy'))
Outputs:
- new_dense: float32 [256, 1024], P(('gx', 'gy'))
- new_dense_acc: float32 [256, 1024], P(('gx', 'gy'))
- new_table: float32 [131072, 128], P(('gx', 'gy'))
- new_row_acc: float32 [131072], P(('gx', 'gy'))
The draws below stay inside these ranges and needn't reach their ends.
Inputs may be any that keep to these rules, and one draw needn't show every extreme that they name: `touched`: within one device's 512 entries no row number repeats.
All inputs are finite; a program needn't handle non-finite values.
Results may differ from the reference program's by a relative error of at most 0.000022.
Values sent between devices are 32-bit elements; how exact they have to be, the bound alone decides.
A program may use at most 128 MiB of HBM per device.

```python
import jax
import jax.numpy as jnp
from jax import lax

H = 1024
EMB_DIM = 128
ROWS_DEV = 4096
TOUCH_DEV = 512
SHARDS = 32
DENSE_ROWS = 256
TABLE_ROWS = 131072
TOUCHED = 16384


def draw_touched(key, part):
    keys = jax.random.split(jax.random.fold_in(key, 11), SHARDS)
    picks = jax.vmap(lambda single: jax.random.permutation(single, ROWS_DEV)[:TOUCH_DEV])(keys)
    return picks.reshape(TOUCHED).astype(jnp.int32)


def draw_emb_grads(key, part):
    first = jax.random.fold_in(jax.random.fold_in(key, 23), 0)
    owner = jnp.arange(TOUCHED, dtype=jnp.float32) // TOUCH_DEV
    ramp = 1.0 + 2.0 * owner / max(SHARDS - 1, 1)
    values = jax.random.normal(first, (TOUCHED, EMB_DIM), jnp.float32)
    scale = ramp / (8.0 * jnp.sqrt(jnp.float32(SHARDS)))
    return (values * scale[:, None]).astype(jnp.float32)


def draw_dense_acc(key, part):
    logs = jax.random.uniform(jax.random.fold_in(key, 37), (DENSE_ROWS, H), jnp.float32, jnp.log(0.0005), jnp.log(0.05))
    return (jnp.exp(logs) / jnp.float32(SHARDS)).astype(jnp.float32)


def draw_row_acc(key, part):
    logs = jax.random.uniform(jax.random.fold_in(key, 41), (TABLE_ROWS,), jnp.float32, jnp.log(1e-05), jnp.log(0.001))
    return (jnp.exp(logs) / jnp.float32(SHARDS)).astype(jnp.float32)


def spiked(drawn, rng, source, target, shards_of, factor):
    owner, partner = [(jnp.arange(drawn.shape[dim]) // (drawn.shape[dim] // shards_of)).reshape([-1 if axis == dim else 1 for axis in range(drawn.ndim)]) for dim in (source, target)]
    chosen = jax.random.permutation(rng, shards_of)[partner]
    strong = (owner == chosen) | (owner == (partner + shards_of // 2) % shards_of)
    return jnp.where(strong, factor * drawn, drawn)


def steps_of(key, dims, cuts, smallest, top_value):
    loudness, own = 1.0, jax.random.fold_in(key, 6)
    for position, shards_of in cuts:
        heights = jnp.exp(jax.random.uniform(jax.random.fold_in(own, position), (shards_of,), jnp.float32, smallest / len(cuts), top_value / len(cuts)))
        loudness = loudness * jnp.repeat(heights, dims[position] // shards_of).reshape([-1 if axis == position else 1 for axis in range(len(dims))])
    return loudness


def centred(stream_key, shape, scale, most, pieces=(), kind=jnp.bfloat16):
    drawn = scale * jax.random.normal(stream_key, shape, jnp.float32)
    if pieces:
        drawn = drawn * steps_of(stream_key, shape, pieces, -0.22, 0.18)
    return jnp.clip(drawn, -most, most).astype(kind)


def noise_with(rng, dims, scale, most, cuts, heavy, kind=jnp.bfloat16):
    result = scale * jax.random.normal(rng, dims, jnp.float32)
    if cuts:
        result = result * steps_of(rng, dims, cuts, -0.22, 0.18)
    return jnp.clip(spiked(result, jax.random.fold_in(rng, 3), *heavy), -most, most).astype(kind)


def setup_inputs(seed: int = 0) -> dict:
    key_list = jax.random.split(jax.random.key(seed), 8)
    return {
        "dense_grads": noise_with(key_list[0], (SHARDS, DENSE_ROWS, H), 1.0, 6.0, ((0, 32),), (0, 1, 32, 2.75), jnp.float32),
        "dense_param": centred(key_list[1], (DENSE_ROWS, H), 1.0, 6.0, ((0, 32),), jnp.float32),
        "dense_acc": draw_dense_acc(jax.random.fold_in(key_list[7], 71), 0),
        "table": centred(key_list[3], (TABLE_ROWS, EMB_DIM), 1.0, 6.0, ((0, 32),), jnp.float32),
        "row_acc": draw_row_acc(jax.random.fold_in(key_list[7], 71), 0),
        "touched": draw_touched(jax.random.fold_in(key_list[7], 71), 0),
        "emb_grads": draw_emb_grads(jax.random.fold_in(key_list[7], 71), 0),
    }


learn_rate = 0.5
max_norm = 8.0
epsilon = 1e-10

def reference(dense_grads, dense_param, dense_acc, table, row_acc, touched, emb_grads):
    mean_grad = lax.optimization_barrier(jnp.sum(dense_grads, axis=0)) / jnp.float32(SHARDS)
    norm_sq = jnp.sum(mean_grad * mean_grad) + jnp.sum(emb_grads * emb_grads)
    clip = jnp.minimum(jnp.float32(1.0), max_norm / (jnp.sqrt(norm_sq) + 1e-06))
    scaled = clip * mean_grad
    new_dense_acc = dense_acc + scaled * scaled
    new_dense = dense_param - learn_rate * scaled / (jnp.sqrt(new_dense_acc) + epsilon)
    owner = (jnp.arange(TOUCHED, dtype=jnp.int32) // TOUCH_DEV).astype(jnp.int32)
    global_rows = (owner * ROWS_DEV + touched).astype(jnp.int32)
    row_grads = clip * emb_grads
    square_mean = lax.optimization_barrier(jnp.mean(row_grads * row_grads, axis=1))
    updated_acc = row_acc[global_rows] + square_mean
    new_row_acc = row_acc.at[global_rows].set(updated_acc)
    updated_rows = table[global_rows] - learn_rate * row_grads / (jnp.sqrt(updated_acc) + epsilon)[:, None]
    new_table = table.at[global_rows].set(updated_rows)
    return (new_dense, new_dense_acc, new_table, new_row_acc)
```

```python
import functools

import jax
import jax.numpy as jnp
from jax import lax
from jax.experimental import pallas as pl
from jax.experimental.pallas import tpu as pltpu
from jax.sharding import PartitionSpec as P

learn_rate = 0.5
max_norm = 8.0
epsilon = 1e-10

MESH = pl.DeviceIdType.MESH
LANES = 128
UNROLL = 16


def flip(index, mask, size):
    result, bit = 0, 1
    while bit < size:
        digit = (index // bit) % 2
        result = result + bit * ((1 - digit) if mask & bit else digit)
        bit *= 2
    return result


def exchange(
    dims,
    grads,
    emb,
    racc,
    touched,
    mean_out,
    clip_out,
    lane_out,
    acc_out,
    own,
    pair_in,
    sums,
    plane_in,
    line_send,
    line_in,
    norms,
    load_sem,
    pair_send_sem,
    pair_sem,
    plane_send_sem,
    plane_sem,
    line_send_sem,
    line_sem,
    norm_send_sem,
    norm_sem,
):
    slows, fasts, ys, cores = dims
    gx, gy = lax.axis_index("gx"), lax.axis_index("gy")
    slow, fast = gx // fasts, gx % fasts
    y, core = gy // cores, gy % cores
    other = 1 - core
    plane = [(a, b) for a in reversed(range(fasts)) for b in reversed(range(ys)) if a or b]
    order = list(reversed(range(slows)))

    loads = {}
    for k in order:
        loads[k] = pltpu.make_async_copy(grads.at[flip(slow, k, slows)], own.at[k], load_sem.at[k])
        loads[k].start()

    barrier = pltpu.get_barrier_semaphore()
    greet = [(gx, y * cores + other)]
    for a, b in plane:
        greet.append((slow * fasts + flip(fast, a, fasts), flip(y, b, ys) * cores + core))
    for k in range(1, slows):
        greet.append((flip(slow, k, slows) * fasts + fast, gy))
    for device in greet:
        pl.semaphore_signal(barrier, inc=1, device_id=device, device_id_type=MESH)
    pl.semaphore_wait(barrier, len(greet))

    pair = {}
    for k in order:
        loads[k].wait()
        pair[k] = pltpu.make_async_remote_copy(
            src_ref=own.at[k, :, :, other],
            dst_ref=pair_in.at[k],
            send_sem=pair_send_sem.at[k],
            recv_sem=pair_sem.at[k],
            device_id=(gx, y * cores + other),
            device_id_type=MESH,
        )
        pair[k].start()

    across = {}
    for k in order:
        pair[k].wait_recv()
        for a in range(fasts):
            for b in range(ys):
                f, v = flip(fast, a, fasts), flip(y, b, ys)
                sums[k, a * ys + b] = own[k, f, v, core] + pair_in[k, f, v]
        for a, b in plane:
            q = a * ys + b
            across[k, q] = pltpu.make_async_remote_copy(
                src_ref=sums.at[k, q],
                dst_ref=plane_in.at[k, q],
                send_sem=plane_send_sem.at[k, q],
                recv_sem=plane_sem.at[k, q],
                device_id=(slow * fasts + flip(fast, a, fasts), flip(y, b, ys) * cores + core),
                device_id_type=MESH,
            )
            across[k, q].start()

    lane = lax.broadcasted_iota(jnp.int32, (1, LANES), 1)

    def gather(step, carry):
        for i in range(UNROLL):
            t = step * UNROLL + i
            row = touched[t]
            here = lane == row % LANES
            lane_out[pl.ds(t, 1), :] = jnp.where(here, 1.0, 0.0)
            acc_out[pl.ds(t, 1), :] = jnp.where(here, racc[pl.ds(row // LANES, 1), :], 0.0)
        return carry

    lax.fori_loop(0, touched.shape[0] // UNROLL, gather, 0)
    values = emb[...]
    emb_square = jnp.sum(values * values, axis=0, keepdims=True)

    def plane_total(k):
        total = sums[k, 0]
        for a, b in plane:
            across[k, a * ys + b].wait_recv()
            total = total + plane_in[k, a * ys + b]
        return total

    line = {}
    for k in order[:-1]:
        line_send[k] = plane_total(k)
        line[k] = pltpu.make_async_remote_copy(
            src_ref=line_send.at[k],
            dst_ref=line_in.at[k],
            send_sem=line_send_sem.at[k],
            recv_sem=line_sem.at[k],
            device_id=(flip(slow, k, slows) * fasts + fast, gy),
            device_id_type=MESH,
        )
        line[k].start()
    total = plane_total(0)
    for k in order[:-1]:
        line[k].wait_recv()
        total = total + line_in[k]

    shards = slows * fasts * ys * cores
    mean = total / jnp.float32(shards)
    mean_out[...] = mean
    square = mean * mean
    partial = square[:, :LANES]
    for start in range(LANES, square.shape[1], LANES):
        partial = partial + square[:, start : start + LANES]
    norms[0] = jnp.sum(partial, axis=0, keepdims=True) + emb_square

    width, height = slows * fasts, ys * cores
    spread = []
    for k in reversed(range(1, shards)):
        spread.append(
            pltpu.make_async_remote_copy(
                src_ref=norms.at[0],
                dst_ref=norms.at[k],
                send_sem=norm_send_sem,
                recv_sem=norm_sem,
                device_id=(flip(gx, k // height, width), flip(gy, k % height, height)),
                device_id_type=MESH,
            )
        )
        spread[-1].start()
    everyone = pltpu.make_async_copy(
        norms.at[pl.ds(1, shards - 1)], norms.at[pl.ds(1, shards - 1)], norm_sem
    )
    everyone.wait()
    norm_sq = jnp.sum(jnp.sum(norms[...], axis=0), axis=1, keepdims=True)
    clip = jnp.minimum(jnp.float32(1.0), max_norm / (jnp.sqrt(norm_sq) + 1e-06))
    clip_out[...] = jnp.broadcast_to(clip, clip_out.shape)

    for k in order:
        pair[k].wait_send()
    for copy in list(across.values()) + list(line.values()):
        copy.wait_send()
    pltpu.make_async_copy(
        norms.at[pl.ds(1, shards - 1)], norms.at[pl.ds(1, shards - 1)], norm_send_sem
    ).wait()


def update(
    table,
    touched,
    touched_rows,
    clip_ref,
    mean,
    dense_param,
    dense_acc,
    emb,
    lane_hot,
    acc_at,
    racc,
    new_table,
    new_dense,
    new_dense_acc,
    new_racc,
    held,
    change,
    sem,
):
    load = pltpu.make_async_copy(table, held, sem)
    load.start()
    clip = clip_ref[:, :1]
    scaled = clip * mean[...]
    acc = dense_acc[...] + scaled * scaled
    new_dense_acc[...] = acc
    new_dense[...] = dense_param[...] - learn_rate * scaled / (jnp.sqrt(acc) + epsilon)

    row_grads = clip * emb[...]
    width = row_grads.shape[1]
    square_mean = jnp.sum(row_grads * row_grads, axis=1, keepdims=True) / jnp.float32(width)
    updated_acc = jnp.sum(acc_at[...], axis=1, keepdims=True) + square_mean
    change[...] = learn_rate * row_grads / (jnp.sqrt(updated_acc) + epsilon)

    placed = lane_hot[...] * square_mean
    groups = lax.broadcasted_iota(jnp.int32, racc.shape, 0)
    added = racc[...]
    for part in range(touched_rows.shape[0]):
        rows = touched_rows[part : part + 1, :]
        hot = jnp.where(groups == rows // LANES, 1.0, 0.0)
        added = added + jnp.dot(
            hot,
            placed[part * LANES : (part + 1) * LANES],
            precision=lax.Precision.HIGHEST,
            preferred_element_type=jnp.float32,
        )
    new_racc[...] = added
    load.wait()

    def scatter(step, carry):
        base = step * UNROLL
        rows = [touched[base + i] for i in range(UNROLL)]
        fresh = [held[pl.ds(rows[i], 1), :] - change[pl.ds(base + i, 1), :] for i in range(UNROLL)]
        for i in range(UNROLL):
            held[pl.ds(rows[i], 1), :] = fresh[i]
        return carry

    lax.fori_loop(0, touched.shape[0] // UNROLL, scatter, 0)
    store = pltpu.make_async_copy(held, new_table, sem)
    store.start()
    store.wait()


def body(dims, dense_grads, dense_param, dense_acc, table, row_acc, touched, emb_grads):
    slows, fasts, ys, cores = dims
    shards = slows * fasts * ys * cores
    rows, wide = dense_param.shape
    f32 = jnp.float32
    count, width = emb_grads.shape
    grads = dense_grads.reshape(slows, fasts, ys, cores, rows, wide)
    racc = row_acc.reshape(-1, LANES)
    touched_rows = touched.reshape(-1, LANES)
    vmem = pl.BlockSpec(memory_space=pltpu.VMEM)
    smem = pl.BlockSpec(memory_space=pltpu.SMEM)
    hbm = pl.BlockSpec(memory_space=pl.ANY)
    quad = fasts * ys
    dma = pltpu.SemaphoreType.DMA
    block = jax.ShapeDtypeStruct((rows, wide), f32)
    per_row = jax.ShapeDtypeStruct((count, LANES), f32)
    mean, clip, lane_hot, acc_at = pl.pallas_call(
        functools.partial(exchange, dims),
        name="exchange",
        out_shape=(block, jax.ShapeDtypeStruct((1, LANES), f32), per_row, per_row),
        in_specs=[hbm, vmem, vmem, smem],
        out_specs=(vmem,) * 4,
        scratch_shapes=[
            pltpu.VMEM((slows, fasts, ys, cores, rows, wide), f32),
            pltpu.VMEM((slows, fasts, ys, rows, wide), f32),
            pltpu.VMEM((slows, quad, rows, wide), f32),
            pltpu.VMEM((slows, quad, rows, wide), f32),
            pltpu.VMEM((slows, rows, wide), f32),
            pltpu.VMEM((slows, rows, wide), f32),
            pltpu.VMEM((shards, 1, LANES), f32),
            dma((slows,)),
            dma((slows,)),
            dma((slows,)),
            dma((slows, quad)),
            dma((slows, quad)),
            dma((slows,)),
            dma((slows,)),
            dma,
            dma,
        ],
        compiler_params=pltpu.CompilerParams(collective_id=0, has_side_effects=True),
    )(grads, emb_grads, racc, touched)
    new_table, new_dense, new_dense_acc, new_racc = pl.pallas_call(
        update,
        name="update",
        out_shape=(
            jax.ShapeDtypeStruct(table.shape, f32),
            block,
            block,
            jax.ShapeDtypeStruct(racc.shape, f32),
        ),
        in_specs=[hbm, smem] + [vmem] * 9,
        out_specs=(hbm, vmem, vmem, vmem),
        scratch_shapes=[
            pltpu.VMEM(table.shape, f32),
            pltpu.VMEM((count, width), f32),
            dma,
        ],
    )(table, touched, touched_rows, clip, mean, dense_param, dense_acc, emb_grads, lane_hot, acc_at, racc)
    return new_dense, new_dense_acc, new_table, new_racc.reshape(-1)


def solution(mesh):
    wide, high = mesh.shape["gx"], mesh.shape["gy"]
    dims = (wide // 2, 2, high // 2, 2)
    return jax.shard_map(
        functools.partial(body, dims),
        mesh=mesh,
        in_specs=(
            P(("gx", "gy"), None, None),
            P(("gx", "gy"), None),
            P(("gx", "gy"), None),
            P(("gx", "gy"), None),
            P(("gx", "gy")),
            P(("gx", "gy")),
            P(("gx", "gy"), None),
        ),
        out_specs=(
            P(("gx", "gy"), None),
            P(("gx", "gy"), None),
            P(("gx", "gy"), None),
            P(("gx", "gy")),
        ),
        check_vma=False,
    )
```

```python
import functools

import jax
import jax.numpy as jnp
from jax import lax
from jax.experimental import pallas as pl
from jax.experimental.pallas import tpu as pltpu
from jax.sharding import PartitionSpec as P

learn_rate = 0.5
max_norm = 8.0
epsilon = 1e-10

MESH = pl.DeviceIdType.MESH
LANES = 128
UNROLL = 16


def flip(index, mask, size):
    result, bit = 0, 1
    while bit < size:
        digit = (index // bit) % 2
        result = result + bit * ((1 - digit) if mask & bit else digit)
        bit *= 2
    return result


def exchange(
    dims,
    grads,
    emb_hbm,
    racc_hbm,
    touched_hbm,
    table_hbm,
    param_hbm,
    dense_acc_hbm,
    mean_out,
    clip_out,
    lane_out,
    acc_out,
    table_out,
    emb,
    racc,
    param_out,
    dense_acc_out,
    own,
    pair_in,
    sums,
    plane_in,
    line_send,
    line_in,
    norms,
    touched,
    load_sem,
    pair_send_sem,
    pair_sem,
    plane_send_sem,
    plane_sem,
    line_send_sem,
    line_sem,
    norm_send_sem,
    norm_sem,
    side_sem,
):
    slows, fasts, ys, cores = dims
    gx, gy = lax.axis_index("gx"), lax.axis_index("gy")
    slow, fast = gx // fasts, gx % fasts
    y, core = gy // cores, gy % cores
    other = 1 - core
    plane = [(a, b) for a in reversed(range(fasts)) for b in reversed(range(ys)) if a or b]
    order = list(reversed(range(slows)))

    loads = {}
    for k in order:
        loads[k] = pltpu.make_async_copy(grads.at[flip(slow, k, slows)], own.at[k], load_sem.at[k])
        loads[k].start()
    sides = []
    held = (
        (touched_hbm, touched),
        (racc_hbm, racc),
        (emb_hbm, emb),
        (param_hbm, param_out),
        (dense_acc_hbm, dense_acc_out),
        (table_hbm, table_out),
    )
    for n, (source, target) in enumerate(held):
        sides.append(pltpu.make_async_copy(source, target, side_sem.at[n]))
        sides[-1].start()

    barrier = pltpu.get_barrier_semaphore()
    greet = [(gx, y * cores + other)]
    for a, b in plane:
        greet.append((slow * fasts + flip(fast, a, fasts), flip(y, b, ys) * cores + core))
    for k in range(1, slows):
        greet.append((flip(slow, k, slows) * fasts + fast, gy))
    for device in greet:
        pl.semaphore_signal(barrier, inc=1, device_id=device, device_id_type=MESH)
    pl.semaphore_wait(barrier, len(greet))

    pair = {}
    for k in order:
        loads[k].wait()
        pair[k] = pltpu.make_async_remote_copy(
            src_ref=own.at[k, :, :, other],
            dst_ref=pair_in.at[k],
            send_sem=pair_send_sem.at[k],
            recv_sem=pair_sem.at[k],
            device_id=(gx, y * cores + other),
            device_id_type=MESH,
        )
        pair[k].start()

    across = {}
    for k in order:
        pair[k].wait_recv()
        for a in range(fasts):
            for b in range(ys):
                f, v = flip(fast, a, fasts), flip(y, b, ys)
                sums[k, a * ys + b] = own[k, f, v, core] + pair_in[k, f, v]
        for a, b in plane:
            q = a * ys + b
            across[k, q] = pltpu.make_async_remote_copy(
                src_ref=sums.at[k, q],
                dst_ref=plane_in.at[k, q],
                send_sem=plane_send_sem.at[k, q],
                recv_sem=plane_sem.at[k, q],
                device_id=(slow * fasts + flip(fast, a, fasts), flip(y, b, ys) * cores + core),
                device_id_type=MESH,
            )
            across[k, q].start()

    for side in sides[:3]:
        side.wait()
    lane = lax.broadcasted_iota(jnp.int32, (1, LANES), 1)

    def gather(step, carry):
        for i in range(UNROLL):
            t = step * UNROLL + i
            row = touched[t]
            here = lane == row % LANES
            lane_out[pl.ds(t, 1), :] = jnp.where(here, 1.0, 0.0)
            acc_out[pl.ds(t, 1), :] = jnp.where(here, racc[pl.ds(row // LANES, 1), :], 0.0)
        return carry

    lax.fori_loop(0, touched.shape[0] // UNROLL, gather, 0)
    values = emb[...]
    emb_square = jnp.sum(values * values, axis=0, keepdims=True)

    def plane_total(k):
        total = sums[k, 0]
        for a, b in plane:
            across[k, a * ys + b].wait_recv()
            total = total + plane_in[k, a * ys + b]
        return total

    line = {}
    for k in order[:-1]:
        line_send[k] = plane_total(k)
        line[k] = pltpu.make_async_remote_copy(
            src_ref=line_send.at[k],
            dst_ref=line_in.at[k],
            send_sem=line_send_sem.at[k],
            recv_sem=line_sem.at[k],
            device_id=(flip(slow, k, slows) * fasts + fast, gy),
            device_id_type=MESH,
        )
        line[k].start()
    total = plane_total(0)
    for k in order[:-1]:
        line[k].wait_recv()
        total = total + line_in[k]

    shards = slows * fasts * ys * cores
    mean = total / jnp.float32(shards)
    mean_out[...] = mean
    square = mean * mean
    partial = square[:, :LANES]
    for start in range(LANES, square.shape[1], LANES):
        partial = partial + square[:, start : start + LANES]
    norms[0] = jnp.sum(partial, axis=0, keepdims=True) + emb_square

    width, height = slows * fasts, ys * cores
    spread = []
    for k in reversed(range(1, shards)):
        spread.append(
            pltpu.make_async_remote_copy(
                src_ref=norms.at[0],
                dst_ref=norms.at[k],
                send_sem=norm_send_sem,
                recv_sem=norm_sem,
                device_id=(flip(gx, k // height, width), flip(gy, k % height, height)),
                device_id_type=MESH,
            )
        )
        spread[-1].start()
    everyone = pltpu.make_async_copy(
        norms.at[pl.ds(1, shards - 1)], norms.at[pl.ds(1, shards - 1)], norm_sem
    )
    everyone.wait()
    norm_sq = jnp.sum(jnp.sum(norms[...], axis=0), axis=1, keepdims=True)
    clip = jnp.minimum(jnp.float32(1.0), max_norm / (jnp.sqrt(norm_sq) + 1e-06))
    clip_out[...] = jnp.broadcast_to(clip, clip_out.shape)

    for side in sides[3:]:
        side.wait()
    for k in order:
        pair[k].wait_send()
    for copy in list(across.values()) + list(line.values()):
        copy.wait_send()
    pltpu.make_async_copy(
        norms.at[pl.ds(1, shards - 1)], norms.at[pl.ds(1, shards - 1)], norm_send_sem
    ).wait()


def update(
    table,
    touched,
    touched_rows,
    clip_ref,
    mean,
    dense_param,
    dense_acc,
    emb,
    lane_hot,
    acc_at,
    racc,
    held,
    new_table,
    new_dense,
    new_dense_acc,
    new_racc,
    change,
    dense_v,
    acc_v,
    racc_v,
    sems,
):
    clip = clip_ref[:, :1]
    count, width = emb.shape

    def prepare(step, carry):
        part = pl.ds(pl.multiple_of(step * LANES, LANES), LANES)
        row_grads = clip * emb[part, :]
        square_mean = jnp.sum(row_grads * row_grads, axis=1, keepdims=True) / jnp.float32(width)
        updated_acc = jnp.sum(acc_at[part, :], axis=1, keepdims=True) + square_mean
        change[part, :] = learn_rate * row_grads / (jnp.sqrt(updated_acc) + epsilon)
        placed = lane_hot[part, :] * square_mean
        hot = jnp.where(groups == touched_rows[pl.ds(step, 1), :] // LANES, 1.0, 0.0)
        racc_v[...] += jnp.dot(
            hot,
            placed,
            precision=lax.Precision.HIGHEST,
            preferred_element_type=jnp.float32,
        )
        return carry

    groups = lax.broadcasted_iota(jnp.int32, racc.shape, 0)
    racc_v[...] = racc[...]
    for step in range(count // LANES):
        prepare(step, 0)
    def scatter(step, carry):
        base = step * UNROLL
        rows = [touched[base + i] for i in range(UNROLL)]
        fresh = [held[pl.ds(rows[i], 1), :] - change[pl.ds(base + i, 1), :] for i in range(UNROLL)]
        for i in range(UNROLL):
            held[pl.ds(rows[i], 1), :] = fresh[i]
        return carry

    lax.fori_loop(0, touched.shape[0] // UNROLL, scatter, 0)
    stores = [pltpu.make_async_copy(held, new_table, sems.at[0])]
    stores[0].start()

    scaled = clip * mean[...]
    acc = dense_acc[...] + scaled * scaled
    acc_v[...] = acc
    dense_v[...] = dense_param[...] - learn_rate * scaled / (jnp.sqrt(acc) + epsilon)
    pairs = ((racc_v, new_racc), (acc_v, new_dense_acc), (dense_v, new_dense))
    for n, (source, target) in enumerate(pairs):
        stores.append(pltpu.make_async_copy(source, target, sems.at[n + 1]))
        stores[-1].start()
    for store in stores:
        store.wait()


def body(dims, dense_grads, dense_param, dense_acc, table, row_acc, touched, emb_grads):
    slows, fasts, ys, cores = dims
    shards = slows * fasts * ys * cores
    rows, wide = dense_param.shape
    f32 = jnp.float32
    count, width = emb_grads.shape
    grads = dense_grads.reshape(slows, fasts, ys, cores, rows, wide)
    racc = row_acc.reshape(-1, LANES)
    touched_rows = touched.reshape(-1, LANES)
    vmem = pl.BlockSpec(memory_space=pltpu.VMEM)
    smem = pl.BlockSpec(memory_space=pltpu.SMEM)
    hbm = pl.BlockSpec(memory_space=pl.ANY)
    quad = fasts * ys
    dma = pltpu.SemaphoreType.DMA
    block = jax.ShapeDtypeStruct((rows, wide), f32)
    per_row = jax.ShapeDtypeStruct((count, LANES), f32)
    own = (table, emb_grads, racc, dense_param, dense_acc)
    mean, clip, lane_hot, acc_at, held, emb, racc, param, acc = pl.pallas_call(
        functools.partial(exchange, dims),
        name="exchange",
        out_shape=(block, jax.ShapeDtypeStruct((1, LANES), f32), per_row, per_row)
        + tuple(jax.ShapeDtypeStruct(a.shape, f32) for a in own),
        in_specs=[hbm] * 7,
        out_specs=(vmem,) * 9,
        scratch_shapes=[
            pltpu.VMEM((slows, fasts, ys, cores, rows, wide), f32),
            pltpu.VMEM((slows, fasts, ys, rows, wide), f32),
            pltpu.VMEM((slows, quad, rows, wide), f32),
            pltpu.VMEM((slows, quad, rows, wide), f32),
            pltpu.VMEM((slows, rows, wide), f32),
            pltpu.VMEM((slows, rows, wide), f32),
            pltpu.VMEM((shards, 1, LANES), f32),
            pltpu.SMEM((count,), jnp.int32),
            dma((slows,)),
            dma((slows,)),
            dma((slows,)),
            dma((slows, quad)),
            dma((slows, quad)),
            dma((slows,)),
            dma((slows,)),
            dma,
            dma,
            dma((6,)),
        ],
        compiler_params=pltpu.CompilerParams(
            collective_id=0, has_side_effects=True, vmem_limit_bytes=49 << 20
        ),
    )(grads, emb_grads, racc, touched, table, dense_param, dense_acc)
    _, new_table, new_dense, new_dense_acc, new_racc = pl.pallas_call(
        update,
        name="update",
        out_shape=(
            jax.ShapeDtypeStruct(table.shape, f32),
            jax.ShapeDtypeStruct(table.shape, f32),
            block,
            block,
            jax.ShapeDtypeStruct(racc.shape, f32),
        ),
        in_specs=[vmem, smem] + [vmem] * 9,
        out_specs=(vmem,) + (hbm,) * 4,
        input_output_aliases={0: 0},
        scratch_shapes=[
            pltpu.VMEM((count, width), f32),
            pltpu.VMEM((rows, wide), f32),
            pltpu.VMEM((rows, wide), f32),
            pltpu.VMEM(racc.shape, f32),
            dma((4,)),
        ],
        compiler_params=pltpu.CompilerParams(
            vmem_limit_bytes=2 * table.size * 4 + 8 * count * LANES * 4 + (4 << 20)
        ),
    )(held, touched, touched_rows, clip, mean, param, acc, emb, lane_hot, acc_at, racc)
    return new_dense, new_dense_acc, new_table, new_racc.reshape(-1)


def solution(mesh):
    wide, high = mesh.shape["gx"], mesh.shape["gy"]
    dims = (wide // 2, 2, high // 2, 2)
    return jax.shard_map(
        functools.partial(body, dims),
        mesh=mesh,
        in_specs=(
            P(("gx", "gy"), None, None),
            P(("gx", "gy"), None),
            P(("gx", "gy"), None),
            P(("gx", "gy"), None),
            P(("gx", "gy")),
            P(("gx", "gy")),
            P(("gx", "gy"), None),
        ),
        out_specs=(
            P(("gx", "gy"), None),
            P(("gx", "gy"), None),
            P(("gx", "gy"), None),
            P(("gx", "gy")),
        ),
        check_vma=False,
    )
```

```python
import functools

import jax
import jax.numpy as jnp
from jax import lax
from jax.experimental import pallas as pl
from jax.experimental.pallas import tpu as pltpu
from jax.sharding import PartitionSpec as P

learn_rate = 0.5
max_norm = 8.0
epsilon = 1e-10

MESH = pl.DeviceIdType.MESH
LANES = 128
UNROLL = 16


def flip(index, mask, size):
    result, bit = 0, 1
    while bit < size:
        digit = (index // bit) % 2
        result = result + bit * ((1 - digit) if mask & bit else digit)
        bit *= 2
    return result


def exchange(
    dims,
    grads,
    emb_hbm,
    racc_hbm,
    touched_hbm,
    table_hbm,
    param_hbm,
    dense_acc_hbm,
    mean_out,
    clip_out,
    lane_out,
    acc_out,
    table_out,
    emb,
    racc,
    param_out,
    dense_acc_out,
    own,
    pair_in,
    sums,
    plane_in,
    line_send,
    line_in,
    norms,
    touched,
    load_sem,
    pair_send_sem,
    pair_sem,
    plane_send_sem,
    plane_sem,
    line_send_sem,
    line_sem,
    norm_send_sem,
    norm_sem,
    side_sem,
):
    slows, fasts, ys, cores = dims
    gx, gy = lax.axis_index("gx"), lax.axis_index("gy")
    slow, fast = gx // fasts, gx % fasts
    y, core = gy // cores, gy % cores
    other = 1 - core
    plane = [(a, b) for a in reversed(range(fasts)) for b in reversed(range(ys)) if a or b]
    order = list(reversed(range(slows)))

    loads = {}
    for k in order:
        loads[k] = pltpu.make_async_copy(grads.at[flip(slow, k, slows)], own.at[k], load_sem.at[k])
        loads[k].start()
    sides = []
    held = (
        (touched_hbm, touched),
        (racc_hbm, racc),
        (emb_hbm, emb),
        (param_hbm, param_out),
        (dense_acc_hbm, dense_acc_out),
        (table_hbm, table_out),
    )
    for n, (source, target) in enumerate(held):
        sides.append(pltpu.make_async_copy(source, target, side_sem.at[n]))
        sides[-1].start()

    barrier = pltpu.get_barrier_semaphore()
    greet = [(gx, y * cores + other)]
    for a, b in plane:
        greet.append((slow * fasts + flip(fast, a, fasts), flip(y, b, ys) * cores + core))
    for k in range(1, slows):
        greet.append((flip(slow, k, slows) * fasts + fast, gy))
    for device in greet:
        pl.semaphore_signal(barrier, inc=1, device_id=device, device_id_type=MESH)
    pl.semaphore_wait(barrier, len(greet))

    pair = {}
    for k in order:
        loads[k].wait()
        pair[k] = pltpu.make_async_remote_copy(
            src_ref=own.at[k, :, :, other],
            dst_ref=pair_in.at[k],
            send_sem=pair_send_sem.at[k],
            recv_sem=pair_sem.at[k],
            device_id=(gx, y * cores + other),
            device_id_type=MESH,
        )
        pair[k].start()

    across = {}
    for k in order:
        pair[k].wait_recv()
        for a in range(fasts):
            for b in range(ys):
                f, v = flip(fast, a, fasts), flip(y, b, ys)
                sums[k, a * ys + b] = own[k, f, v, core] + pair_in[k, f, v]
        for a, b in plane:
            q = a * ys + b
            across[k, q] = pltpu.make_async_remote_copy(
                src_ref=sums.at[k, q],
                dst_ref=plane_in.at[k, q],
                send_sem=plane_send_sem.at[k, q],
                recv_sem=plane_sem.at[k, q],
                device_id=(slow * fasts + flip(fast, a, fasts), flip(y, b, ys) * cores + core),
                device_id_type=MESH,
            )
            across[k, q].start()

    for side in sides[:3]:
        side.wait()
    lane = lax.broadcasted_iota(jnp.int32, (1, LANES), 1)

    def gather(step, carry):
        for i in range(UNROLL):
            t = step * UNROLL + i
            row = touched[t]
            here = lane == row % LANES
            lane_out[pl.ds(t, 1), :] = jnp.where(here, 1.0, 0.0)
            acc_out[pl.ds(t, 1), :] = jnp.where(here, racc[pl.ds(row // LANES, 1), :], 0.0)
        return carry

    lax.fori_loop(0, touched.shape[0] // UNROLL, gather, 0)
    values = emb[...]
    emb_square = jnp.sum(values * values, axis=0, keepdims=True)

    def plane_total(k):
        total = sums[k, 0]
        for a, b in plane:
            across[k, a * ys + b].wait_recv()
            total = total + plane_in[k, a * ys + b]
        return total

    line = {}
    for k in order[:-1]:
        line_send[k] = plane_total(k)
        line[k] = pltpu.make_async_remote_copy(
            src_ref=line_send.at[k],
            dst_ref=line_in.at[k],
            send_sem=line_send_sem.at[k],
            recv_sem=line_sem.at[k],
            device_id=(flip(slow, k, slows) * fasts + fast, gy),
            device_id_type=MESH,
        )
        line[k].start()
    total = plane_total(0)
    for k in order[:-1]:
        line[k].wait_recv()
        total = total + line_in[k]

    shards = slows * fasts * ys * cores
    mean = total / jnp.float32(shards)
    mean_out[...] = mean
    square = mean * mean
    partial = square[:, :LANES]
    for start in range(LANES, square.shape[1], LANES):
        partial = partial + square[:, start : start + LANES]
    norms[0] = jnp.sum(partial, axis=0, keepdims=True) + emb_square

    width, height = slows * fasts, ys * cores
    spread = []
    for k in reversed(range(1, shards)):
        spread.append(
            pltpu.make_async_remote_copy(
                src_ref=norms.at[0],
                dst_ref=norms.at[k],
                send_sem=norm_send_sem,
                recv_sem=norm_sem,
                device_id=(flip(gx, k // height, width), flip(gy, k % height, height)),
                device_id_type=MESH,
            )
        )
        spread[-1].start()
    everyone = pltpu.make_async_copy(
        norms.at[pl.ds(1, shards - 1)], norms.at[pl.ds(1, shards - 1)], norm_sem
    )
    everyone.wait()
    norm_sq = jnp.sum(jnp.sum(norms[...], axis=0), axis=1, keepdims=True)
    clip = jnp.minimum(jnp.float32(1.0), max_norm / (jnp.sqrt(norm_sq) + 1e-06))
    clip_out[...] = jnp.broadcast_to(clip, clip_out.shape)

    for side in sides[3:]:
        side.wait()
    for k in order:
        pair[k].wait_send()
    for copy in list(across.values()) + list(line.values()):
        copy.wait_send()
    pltpu.make_async_copy(
        norms.at[pl.ds(1, shards - 1)], norms.at[pl.ds(1, shards - 1)], norm_send_sem
    ).wait()


def update(
    table,
    touched,
    touched_rows,
    clip_ref,
    mean,
    dense_param,
    dense_acc,
    emb,
    lane_hot,
    acc_at,
    racc,
    held,
    new_table,
    new_dense,
    new_dense_acc,
    new_racc,
    change,
    dense_v,
    acc_v,
    racc_v,
    sems,
):
    clip = clip_ref[:, :1]
    count, width = emb.shape

    def prepare(step, carry):
        part = pl.ds(pl.multiple_of(step * LANES, LANES), LANES)
        row_grads = clip * emb[part, :]
        square_mean = jnp.sum(row_grads * row_grads, axis=1, keepdims=True) / jnp.float32(width)
        updated_acc = jnp.sum(acc_at[part, :], axis=1, keepdims=True) + square_mean
        change[part, :] = learn_rate * row_grads / (jnp.sqrt(updated_acc) + epsilon)
        placed = lane_hot[part, :] * square_mean
        hot = jnp.where(groups == touched_rows[pl.ds(step, 1), :] // LANES, 1.0, 0.0)
        racc_v[...] += jnp.dot(
            hot,
            placed,
            precision=lax.Precision.HIGHEST,
            preferred_element_type=jnp.float32,
        )
        return carry

    groups = lax.broadcasted_iota(jnp.int32, racc.shape, 0)
    racc_v[...] = racc[...]
    for step in range(count // LANES):
        prepare(step, 0)
    def scatter(step, carry):
        base = step * UNROLL
        rows = [touched[base + i] for i in range(UNROLL)]
        fresh = [held[pl.ds(rows[i], 1), :] - change[pl.ds(base + i, 1), :] for i in range(UNROLL)]
        for i in range(UNROLL):
            held[pl.ds(rows[i], 1), :] = fresh[i]
        return carry

    lax.fori_loop(0, touched.shape[0] // UNROLL, scatter, 0)
    stores = [pltpu.make_async_copy(held, new_table, sems.at[0])]
    stores[0].start()

    scaled = clip * mean[...]
    acc = dense_acc[...] + scaled * scaled
    acc_v[...] = acc
    dense_v[...] = dense_param[...] - learn_rate * scaled / (jnp.sqrt(acc) + epsilon)
    pairs = ((racc_v, new_racc), (acc_v, new_dense_acc), (dense_v, new_dense))
    for n, (source, target) in enumerate(pairs):
        stores.append(pltpu.make_async_copy(source, target, sems.at[n + 1]))
        stores[-1].start()
    for store in stores:
        store.wait()


def body(dims, dense_grads, dense_param, dense_acc, table, row_acc, touched, emb_grads):
    slows, fasts, ys, cores = dims
    shards = slows * fasts * ys * cores
    rows, wide = dense_param.shape
    f32 = jnp.float32
    count, width = emb_grads.shape
    grads = dense_grads.reshape(slows, fasts, ys, cores, rows, wide)
    racc = row_acc.reshape(-1, LANES)
    touched_rows = touched.reshape(-1, LANES)
    vmem = pl.BlockSpec(memory_space=pltpu.VMEM)
    smem = pl.BlockSpec(memory_space=pltpu.SMEM)
    hbm = pl.BlockSpec(memory_space=pl.ANY)
    quad = fasts * ys
    dma = pltpu.SemaphoreType.DMA
    block = jax.ShapeDtypeStruct((rows, wide), f32)
    per_row = jax.ShapeDtypeStruct((count, LANES), f32)
    own = (table, emb_grads, racc, dense_param, dense_acc)
    mean, clip, lane_hot, acc_at, held, emb, racc, param, acc = pl.pallas_call(
        functools.partial(exchange, dims),
        name="exchange",
        out_shape=(block, jax.ShapeDtypeStruct((1, LANES), f32), per_row, per_row)
        + tuple(jax.ShapeDtypeStruct(a.shape, f32) for a in own),
        in_specs=[pl.BlockSpec(memory_space=pltpu.HBM)] * 7,
        out_specs=(vmem,) * 9,
        scratch_shapes=[
            pltpu.VMEM((slows, fasts, ys, cores, rows, wide), f32),
            pltpu.VMEM((slows, fasts, ys, rows, wide), f32),
            pltpu.VMEM((slows, quad, rows, wide), f32),
            pltpu.VMEM((slows, quad, rows, wide), f32),
            pltpu.VMEM((slows, rows, wide), f32),
            pltpu.VMEM((slows, rows, wide), f32),
            pltpu.VMEM((shards, 1, LANES), f32),
            pltpu.SMEM((count,), jnp.int32),
            dma((slows,)),
            dma((slows,)),
            dma((slows,)),
            dma((slows, quad)),
            dma((slows, quad)),
            dma((slows,)),
            dma((slows,)),
            dma,
            dma,
            dma((6,)),
        ],
        compiler_params=pltpu.CompilerParams(
            collective_id=0, has_side_effects=True, vmem_limit_bytes=49 << 20
        ),
    )(*[pltpu.with_memory_space_constraint(a, pltpu.HBM) for a in (grads, emb_grads, racc, touched, table, dense_param, dense_acc)])
    _, new_table, new_dense, new_dense_acc, new_racc = pl.pallas_call(
        update,
        name="update",
        out_shape=(
            jax.ShapeDtypeStruct(table.shape, f32),
            jax.ShapeDtypeStruct(table.shape, f32),
            block,
            block,
            jax.ShapeDtypeStruct(racc.shape, f32),
        ),
        in_specs=[vmem, smem] + [vmem] * 9,
        out_specs=(vmem,) + (hbm,) * 4,
        input_output_aliases={0: 0},
        scratch_shapes=[
            pltpu.VMEM((count, width), f32),
            pltpu.VMEM((rows, wide), f32),
            pltpu.VMEM((rows, wide), f32),
            pltpu.VMEM(racc.shape, f32),
            dma((4,)),
        ],
        compiler_params=pltpu.CompilerParams(
            vmem_limit_bytes=2 * table.size * 4 + 8 * count * LANES * 4 + (4 << 20)
        ),
    )(held, touched, touched_rows, clip, mean, param, acc, emb, lane_hot, acc_at, racc)
    return new_dense, new_dense_acc, new_table, new_racc.reshape(-1)


def solution(mesh):
    wide, high = mesh.shape["gx"], mesh.shape["gy"]
    dims = (wide // 2, 2, high // 2, 2)
    return jax.shard_map(
        functools.partial(body, dims),
        mesh=mesh,
        in_specs=(
            P(("gx", "gy"), None, None),
            P(("gx", "gy"), None),
            P(("gx", "gy"), None),
            P(("gx", "gy"), None),
            P(("gx", "gy")),
            P(("gx", "gy")),
            P(("gx", "gy"), None),
        ),
        out_specs=(
            P(("gx", "gy"), None),
            P(("gx", "gy"), None),
            P(("gx", "gy"), None),
            P(("gx", "gy")),
        ),
        check_vma=False,
    )
```

```python
import functools

import jax
import jax.numpy as jnp
from jax import lax
from jax.experimental import pallas as pl
from jax.experimental.pallas import tpu as pltpu
from jax.sharding import PartitionSpec as P

learn_rate = 0.5
max_norm = 8.0
epsilon = 1e-10

MESH = pl.DeviceIdType.MESH
LANES = 128
UNROLL = 16


def flip(index, mask, size):
    result, bit = 0, 1
    while bit < size:
        digit = (index // bit) % 2
        result = result + bit * ((1 - digit) if mask & bit else digit)
        bit *= 2
    return result


def exchange(
    dims,
    grads,
    emb_hbm,
    racc_hbm,
    touched_hbm,
    table_hbm,
    param_hbm,
    dense_acc_hbm,
    mean_out,
    clip_out,
    lane_out,
    acc_out,
    table_out,
    emb,
    racc,
    param_out,
    dense_acc_out,
    own,
    pair_in,
    sums,
    plane_in,
    line_send,
    line_in,
    norms,
    touched,
    load_sem,
    pair_send_sem,
    pair_sem,
    plane_send_sem,
    plane_sem,
    line_send_sem,
    line_sem,
    norm_send_sem,
    norm_sem,
    side_sem,
):
    slows, fasts, ys, cores = dims
    gx, gy = lax.axis_index("gx"), lax.axis_index("gy")
    slow, fast = gx // fasts, gx % fasts
    y, core = gy // cores, gy % cores
    other = 1 - core
    plane = [(a, b) for a in reversed(range(fasts)) for b in reversed(range(ys)) if a or b]
    order = list(reversed(range(slows)))

    loads = {}
    for k in order:
        loads[k] = pltpu.make_async_copy(grads.at[flip(slow, k, slows)], own.at[k], load_sem.at[k])
        loads[k].start()
    barrier = pltpu.get_barrier_semaphore()
    greet = [(gx, y * cores + other)]
    for a, b in plane:
        greet.append((slow * fasts + flip(fast, a, fasts), flip(y, b, ys) * cores + core))
    for k in range(1, slows):
        greet.append((flip(slow, k, slows) * fasts + fast, gy))
    for device in greet:
        pl.semaphore_signal(barrier, inc=1, device_id=device, device_id_type=MESH)
    pl.semaphore_wait(barrier, len(greet))

    pair = {}
    for k in order:
        loads[k].wait()
        pair[k] = pltpu.make_async_remote_copy(
            src_ref=own.at[k, :, :, other],
            dst_ref=pair_in.at[k],
            send_sem=pair_send_sem.at[k],
            recv_sem=pair_sem.at[k],
            device_id=(gx, y * cores + other),
            device_id_type=MESH,
        )
        pair[k].start()

    sides = []
    held = (
        (emb_hbm, emb),
        (touched_hbm, touched),
        (racc_hbm, racc),
        (param_hbm, param_out),
        (dense_acc_hbm, dense_acc_out),
        (table_hbm, table_out),
    )
    for n, (source, target) in enumerate(held):
        sides.append(pltpu.make_async_copy(source, target, side_sem.at[n]))
        sides[-1].start()

    across = {}
    for k in order:
        pair[k].wait_recv()
        for a in range(fasts):
            for b in range(ys):
                f, v = flip(fast, a, fasts), flip(y, b, ys)
                sums[k, a * ys + b] = own[k, f, v, core] + pair_in[k, f, v]
        for a, b in plane:
            q = a * ys + b
            across[k, q] = pltpu.make_async_remote_copy(
                src_ref=sums.at[k, q],
                dst_ref=plane_in.at[k, q],
                send_sem=plane_send_sem.at[k, q],
                recv_sem=plane_sem.at[k, q],
                device_id=(slow * fasts + flip(fast, a, fasts), flip(y, b, ys) * cores + core),
                device_id_type=MESH,
            )
            across[k, q].start()

    sides[0].wait()
    values = emb[...]
    emb_square = jnp.sum(values * values, axis=0, keepdims=True)

    def plane_total(k):
        total = sums[k, 0]
        for a, b in plane:
            across[k, a * ys + b].wait_recv()
            total = total + plane_in[k, a * ys + b]
        return total

    line = {}
    for k in order[:-1]:
        line_send[k] = plane_total(k)
        line[k] = pltpu.make_async_remote_copy(
            src_ref=line_send.at[k],
            dst_ref=line_in.at[k],
            send_sem=line_send_sem.at[k],
            recv_sem=line_sem.at[k],
            device_id=(flip(slow, k, slows) * fasts + fast, gy),
            device_id_type=MESH,
        )
        line[k].start()
    total = plane_total(0)
    for k in order[:-1]:
        line[k].wait_recv()
        total = total + line_in[k]

    shards = slows * fasts * ys * cores
    mean = total / jnp.float32(shards)
    mean_out[...] = mean
    square = mean * mean
    partial = square[:, :LANES]
    for start in range(LANES, square.shape[1], LANES):
        partial = partial + square[:, start : start + LANES]
    norms[0] = jnp.sum(partial, axis=0, keepdims=True) + emb_square

    width, height = slows * fasts, ys * cores
    spread = []
    for k in reversed(range(1, shards)):
        spread.append(
            pltpu.make_async_remote_copy(
                src_ref=norms.at[0],
                dst_ref=norms.at[k],
                send_sem=norm_send_sem,
                recv_sem=norm_sem,
                device_id=(flip(gx, k // height, width), flip(gy, k % height, height)),
                device_id_type=MESH,
            )
        )
        spread[-1].start()
    for side in sides[1:3]:
        side.wait()
    lane = lax.broadcasted_iota(jnp.int32, (1, LANES), 1)

    def gather(step, carry):
        for i in range(UNROLL):
            t = step * UNROLL + i
            row = touched[t]
            here = lane == row % LANES
            lane_out[pl.ds(t, 1), :] = jnp.where(here, 1.0, 0.0)
            acc_out[pl.ds(t, 1), :] = jnp.where(here, racc[pl.ds(row // LANES, 1), :], 0.0)
        return carry

    lax.fori_loop(0, touched.shape[0] // UNROLL, gather, 0)
    for start in range(0, touched.shape[0], LANES):
        part = pl.ds(start, LANES)
        found = jnp.sum(acc_out[part, :], axis=1, keepdims=True)
        acc_out[part, :] = jnp.broadcast_to(found, (LANES, LANES))

    everyone = pltpu.make_async_copy(
        norms.at[pl.ds(1, shards - 1)], norms.at[pl.ds(1, shards - 1)], norm_sem
    )
    everyone.wait()
    norm_sq = jnp.sum(jnp.sum(norms[...], axis=0), axis=1, keepdims=True)
    clip = jnp.minimum(jnp.float32(1.0), max_norm / (jnp.sqrt(norm_sq) + 1e-06))
    clip_out[...] = jnp.broadcast_to(clip, clip_out.shape)

    for side in sides[3:]:
        side.wait()
    for k in order:
        pair[k].wait_send()
    for copy in list(across.values()) + list(line.values()):
        copy.wait_send()
    pltpu.make_async_copy(
        norms.at[pl.ds(1, shards - 1)], norms.at[pl.ds(1, shards - 1)], norm_send_sem
    ).wait()


def update(
    table,
    touched,
    touched_rows,
    clip_ref,
    mean,
    dense_param,
    dense_acc,
    emb,
    lane_hot,
    acc_at,
    racc,
    held,
    new_table,
    new_dense,
    new_dense_acc,
    new_racc,
    change,
    placed,
    dense_v,
    acc_v,
    racc_v,
    sems,
):
    clip = clip_ref[:, :1]
    count, width = emb.shape

    def prepare(start):
        part = pl.ds(start, LANES)
        row_grads = clip * emb[part, :]
        square_mean = jnp.sum(row_grads * row_grads, axis=1, keepdims=True) / jnp.float32(width)
        updated_acc = acc_at[part, :] + square_mean
        change[part, :] = learn_rate * row_grads / (jnp.sqrt(updated_acc) + epsilon)
        placed[part, :] = lane_hot[part, :] * square_mean

    def scatter(start):
        for base in range(start, start + LANES, UNROLL):
            rows = [touched[base + i] for i in range(UNROLL)]
            fresh = [
                held[pl.ds(rows[i], 1), :] - change[pl.ds(base + i, 1), :] for i in range(UNROLL)
            ]
            for i in range(UNROLL):
                held[pl.ds(rows[i], 1), :] = fresh[i]

    starts = range(0, count, LANES)
    prepare(0)
    for start in starts:
        if start + LANES < count:
            prepare(start + LANES)
        scatter(start)
    stores = [pltpu.make_async_copy(held, new_table, sems.at[0])]
    stores[0].start()

    groups = lax.broadcasted_iota(jnp.int32, racc.shape, 0)
    added = racc[...]
    for start in starts:
        rows = touched_rows[start // LANES : start // LANES + 1, :]
        added = added + jnp.dot(
            jnp.where(groups == rows // LANES, 1.0, 0.0),
            placed[start : start + LANES, :],
            precision=lax.Precision.HIGHEST,
            preferred_element_type=jnp.float32,
        )
    racc_v[...] = added
    scaled = clip * mean[...]
    acc = dense_acc[...] + scaled * scaled
    acc_v[...] = acc
    dense_v[...] = dense_param[...] - learn_rate * scaled / (jnp.sqrt(acc) + epsilon)
    pairs = ((racc_v, new_racc), (acc_v, new_dense_acc), (dense_v, new_dense))
    for n, (source, target) in enumerate(pairs):
        stores.append(pltpu.make_async_copy(source, target, sems.at[n + 1]))
        stores[-1].start()
    for store in stores:
        store.wait()


def body(dims, dense_grads, dense_param, dense_acc, table, row_acc, touched, emb_grads):
    slows, fasts, ys, cores = dims
    shards = slows * fasts * ys * cores
    rows, wide = dense_param.shape
    f32 = jnp.float32
    count, width = emb_grads.shape
    grads = dense_grads.reshape(slows, fasts, ys, cores, rows, wide)
    racc = row_acc.reshape(-1, LANES)
    touched_rows = touched.reshape(-1, LANES)
    vmem = pl.BlockSpec(memory_space=pltpu.VMEM)
    smem = pl.BlockSpec(memory_space=pltpu.SMEM)
    hbm = pl.BlockSpec(memory_space=pl.ANY)
    quad = fasts * ys
    dma = pltpu.SemaphoreType.DMA
    block = jax.ShapeDtypeStruct((rows, wide), f32)
    per_row = jax.ShapeDtypeStruct((count, LANES), f32)
    own = (table, emb_grads, racc, dense_param, dense_acc)
    mean, clip, lane_hot, acc_at, held, emb, racc, param, acc = pl.pallas_call(
        functools.partial(exchange, dims),
        name="exchange",
        out_shape=(block, jax.ShapeDtypeStruct((1, LANES), f32), per_row, per_row)
        + tuple(jax.ShapeDtypeStruct(a.shape, f32) for a in own),
        in_specs=[pl.BlockSpec(memory_space=pltpu.HBM)] * 7,
        out_specs=(vmem,) * 9,
        scratch_shapes=[
            pltpu.VMEM((slows, fasts, ys, cores, rows, wide), f32),
            pltpu.VMEM((slows, fasts, ys, rows, wide), f32),
            pltpu.VMEM((slows, quad, rows, wide), f32),
            pltpu.VMEM((slows, quad, rows, wide), f32),
            pltpu.VMEM((slows, rows, wide), f32),
            pltpu.VMEM((slows, rows, wide), f32),
            pltpu.VMEM((shards, 1, LANES), f32),
            pltpu.SMEM((count,), jnp.int32),
            dma((slows,)),
            dma((slows,)),
            dma((slows,)),
            dma((slows, quad)),
            dma((slows, quad)),
            dma((slows,)),
            dma((slows,)),
            dma,
            dma,
            dma((6,)),
        ],
        compiler_params=pltpu.CompilerParams(
            collective_id=0, has_side_effects=True, vmem_limit_bytes=49 << 20
        ),
    )(*[pltpu.with_memory_space_constraint(a, pltpu.HBM) for a in (grads, emb_grads, racc, touched, table, dense_param, dense_acc)])
    _, new_table, new_dense, new_dense_acc, new_racc = pl.pallas_call(
        update,
        name="update",
        out_shape=(
            jax.ShapeDtypeStruct(table.shape, f32),
            jax.ShapeDtypeStruct(table.shape, f32),
            block,
            block,
            jax.ShapeDtypeStruct(racc.shape, f32),
        ),
        in_specs=[vmem, smem] + [vmem] * 9,
        out_specs=(vmem,) + (hbm,) * 4,
        input_output_aliases={0: 0},
        scratch_shapes=[
            pltpu.VMEM((count, width), f32),
            pltpu.VMEM((count, LANES), f32),
            pltpu.VMEM((rows, wide), f32),
            pltpu.VMEM((rows, wide), f32),
            pltpu.VMEM(racc.shape, f32),
            dma((4,)),
        ],
        compiler_params=pltpu.CompilerParams(
            vmem_limit_bytes=2 * table.size * 4 + 8 * count * LANES * 4 + (4 << 20)
        ),
    )(held, touched, touched_rows, clip, mean, param, acc, emb, lane_hot, acc_at, racc)
    return new_dense, new_dense_acc, new_table, new_racc.reshape(-1)


def solution(mesh):
    wide, high = mesh.shape["gx"], mesh.shape["gy"]
    dims = (wide // 2, 2, high // 2, 2)
    return jax.shard_map(
        functools.partial(body, dims),
        mesh=mesh,
        in_specs=(
            P(("gx", "gy"), None, None),
            P(("gx", "gy"), None),
            P(("gx", "gy"), None),
            P(("gx", "gy"), None),
            P(("gx", "gy")),
            P(("gx", "gy")),
            P(("gx", "gy"), None),
        ),
        out_specs=(
            P(("gx", "gy"), None),
            P(("gx", "gy"), None),
            P(("gx", "gy"), None),
            P(("gx", "gy")),
        ),
        check_vma=False,
    )
```

```python
import functools

import jax
import jax.numpy as jnp
from jax import lax
from jax.experimental import pallas as pl
from jax.experimental.pallas import tpu as pltpu
from jax.sharding import PartitionSpec as P

learn_rate = 0.5
max_norm = 8.0
epsilon = 1e-10

MESH = pl.DeviceIdType.MESH
LANES = 128
UNROLL = 16


def flip(index, mask, size):
    result, bit = 0, 1
    while bit < size:
        digit = (index // bit) % 2
        result = result + bit * ((1 - digit) if mask & bit else digit)
        bit *= 2
    return result


def exchange(
    dims,
    grads,
    emb_hbm,
    racc_hbm,
    touched_hbm,
    table_hbm,
    param_hbm,
    dense_acc_hbm,
    mean_out,
    clip_out,
    lane_out,
    acc_out,
    table_out,
    emb,
    racc,
    param_out,
    dense_acc_out,
    own,
    pair_in,
    sums,
    plane_in,
    line_send,
    line_in,
    norms,
    touched,
    load_sem,
    pair_send_sem,
    pair_sem,
    plane_send_sem,
    plane_sem,
    line_send_sem,
    line_sem,
    norm_send_sem,
    norm_sem,
    side_sem,
):
    slows, fasts, ys, cores = dims
    gx, gy = lax.axis_index("gx"), lax.axis_index("gy")
    slow, fast = gx // fasts, gx % fasts
    y, core = gy // cores, gy % cores
    other = 1 - core
    plane = [(a, b) for a in reversed(range(fasts)) for b in reversed(range(ys)) if a or b]
    order = list(reversed(range(slows)))

    loads = {}
    for k in order:
        loads[k] = pltpu.make_async_copy(grads.at[flip(slow, k, slows)], own.at[k], load_sem.at[k])
        loads[k].start()
    barrier = pltpu.get_barrier_semaphore()
    greet = [(gx, y * cores + other)]
    for a, b in plane:
        greet.append((slow * fasts + flip(fast, a, fasts), flip(y, b, ys) * cores + core))
    for k in range(1, slows):
        greet.append((flip(slow, k, slows) * fasts + fast, gy))
    for device in greet:
        pl.semaphore_signal(barrier, inc=1, device_id=device, device_id_type=MESH)
    pl.semaphore_wait(barrier, len(greet))

    pair = {}
    for k in order:
        loads[k].wait()
        pair[k] = pltpu.make_async_remote_copy(
            src_ref=own.at[k, :, :, other],
            dst_ref=pair_in.at[k],
            send_sem=pair_send_sem.at[k],
            recv_sem=pair_sem.at[k],
            device_id=(gx, y * cores + other),
            device_id_type=MESH,
        )
        pair[k].start()

    sides = []
    held = (
        (emb_hbm, emb),
        (touched_hbm, touched),
        (racc_hbm, racc),
        (param_hbm, param_out),
        (dense_acc_hbm, dense_acc_out),
        (table_hbm, table_out),
    )
    for n, (source, target) in enumerate(held):
        sides.append(pltpu.make_async_copy(source, target, side_sem.at[n]))
        sides[-1].start()

    across = {}
    for k in order:
        pair[k].wait_recv()
        for a in range(fasts):
            for b in range(ys):
                f, v = flip(fast, a, fasts), flip(y, b, ys)
                sums[k, a * ys + b] = own[k, f, v, core] + pair_in[k, f, v]
        for a, b in plane:
            q = a * ys + b
            across[k, q] = pltpu.make_async_remote_copy(
                src_ref=sums.at[k, q],
                dst_ref=plane_in.at[k, q],
                send_sem=plane_send_sem.at[k, q],
                recv_sem=plane_sem.at[k, q],
                device_id=(slow * fasts + flip(fast, a, fasts), flip(y, b, ys) * cores + core),
                device_id_type=MESH,
            )
            across[k, q].start()

    sides[0].wait()
    values = emb[...]
    emb_square = jnp.sum(values * values, axis=0, keepdims=True)

    def plane_total(k):
        total = sums[k, 0]
        for a, b in plane:
            across[k, a * ys + b].wait_recv()
            total = total + plane_in[k, a * ys + b]
        return total

    line = {}
    for k in order[:-1]:
        line_send[k] = plane_total(k)
        line[k] = pltpu.make_async_remote_copy(
            src_ref=line_send.at[k],
            dst_ref=line_in.at[k],
            send_sem=line_send_sem.at[k],
            recv_sem=line_sem.at[k],
            device_id=(flip(slow, k, slows) * fasts + fast, gy),
            device_id_type=MESH,
        )
        line[k].start()
    total = plane_total(0)
    for k in order[:-1]:
        line[k].wait_recv()
        total = total + line_in[k]

    shards = slows * fasts * ys * cores
    mean = total / jnp.float32(shards)
    mean_out[...] = mean
    square = mean * mean
    partial = square[:, :LANES]
    for start in range(LANES, square.shape[1], LANES):
        partial = partial + square[:, start : start + LANES]
    norms[0] = jnp.sum(partial, axis=0, keepdims=True) + emb_square

    width, height = slows * fasts, ys * cores
    spread = []
    for k in reversed(range(1, shards)):
        spread.append(
            pltpu.make_async_remote_copy(
                src_ref=norms.at[0],
                dst_ref=norms.at[k],
                send_sem=norm_send_sem,
                recv_sem=norm_sem,
                device_id=(flip(gx, k // height, width), flip(gy, k % height, height)),
                device_id_type=MESH,
            )
        )
        spread[-1].start()
    for side in sides[1:3]:
        side.wait()
    lane = lax.broadcasted_iota(jnp.int32, (1, LANES), 1)

    def gather(step, carry):
        for i in range(UNROLL):
            t = step * UNROLL + i
            row = touched[t]
            here = lane == row % LANES
            lane_out[pl.ds(t, 1), :] = jnp.where(here, 1.0, 0.0)
            acc_out[pl.ds(t, 1), :] = jnp.where(here, racc[pl.ds(row // LANES, 1), :], 0.0)
        return carry

    lax.fori_loop(0, touched.shape[0] // UNROLL, gather, 0)
    for start in range(0, touched.shape[0], LANES):
        part = pl.ds(start, LANES)
        found = jnp.sum(acc_out[part, :], axis=1, keepdims=True)
        acc_out[part, :] = jnp.broadcast_to(found, (LANES, LANES))

    everyone = pltpu.make_async_copy(
        norms.at[pl.ds(1, shards - 1)], norms.at[pl.ds(1, shards - 1)], norm_sem
    )
    everyone.wait()
    norm_sq = jnp.sum(jnp.sum(norms[...], axis=0), axis=1, keepdims=True)
    clip = jnp.minimum(jnp.float32(1.0), max_norm / (jnp.sqrt(norm_sq) + 1e-06))
    clip_out[...] = jnp.broadcast_to(clip, clip_out.shape)

    for side in sides[3:]:
        side.wait()
    for k in order:
        pair[k].wait_send()
    for copy in list(across.values()) + list(line.values()):
        copy.wait_send()
    pltpu.make_async_copy(
        norms.at[pl.ds(1, shards - 1)], norms.at[pl.ds(1, shards - 1)], norm_send_sem
    ).wait()


def update(
    table,
    touched_any,
    touched_rows,
    clip_ref,
    mean,
    dense_param,
    dense_acc,
    emb,
    lane_hot,
    acc_at,
    racc,
    held,
    new_table,
    new_dense,
    new_dense_acc,
    new_racc,
    change,
    placed,
    dense_v,
    acc_v,
    racc_v,
    touched,
    sems,
):
    numbers = pltpu.make_async_copy(touched_any, touched, sems.at[4])
    numbers.start()
    clip = clip_ref[:, :1]
    count, width = emb.shape

    def prepare(start):
        part = pl.ds(start, LANES)
        row_grads = clip * emb[part, :]
        square_mean = jnp.sum(row_grads * row_grads, axis=1, keepdims=True) / jnp.float32(width)
        updated_acc = acc_at[part, :] + square_mean
        change[part, :] = learn_rate * row_grads / (jnp.sqrt(updated_acc) + epsilon)
        placed[part, :] = lane_hot[part, :] * square_mean

    def scatter(start):
        for base in range(start, start + LANES, UNROLL):
            rows = [touched[base + i] for i in range(UNROLL)]
            fresh = [
                held[pl.ds(rows[i], 1), :] - change[pl.ds(base + i, 1), :] for i in range(UNROLL)
            ]
            for i in range(UNROLL):
                held[pl.ds(rows[i], 1), :] = fresh[i]

    starts = range(0, count, LANES)
    ahead = 2
    for start in starts[:ahead]:
        prepare(start)
    numbers.wait()
    for start in starts:
        if start + ahead * LANES < count:
            prepare(start + ahead * LANES)
        scatter(start)
    stores = [pltpu.make_async_copy(held, new_table, sems.at[0])]
    stores[0].start()

    def send(n, source, target):
        stores.append(pltpu.make_async_copy(source, target, sems.at[n]))
        stores[-1].start()

    scaled = clip * mean[...]
    acc = dense_acc[...] + scaled * scaled
    acc_v[...] = acc
    dense_v[...] = dense_param[...] - learn_rate * scaled / (jnp.sqrt(acc) + epsilon)
    send(1, acc_v, new_dense_acc)
    send(2, dense_v, new_dense)

    groups = lax.broadcasted_iota(jnp.int32, racc.shape, 0)
    added = racc[...]
    for start in starts:
        rows = touched_rows[start // LANES : start // LANES + 1, :]
        added = added + jnp.dot(
            jnp.where(groups == rows // LANES, 1.0, 0.0),
            placed[start : start + LANES, :],
            precision=lax.Precision.HIGHEST,
            preferred_element_type=jnp.float32,
        )
    racc_v[...] = added
    send(3, racc_v, new_racc)
    for store in stores:
        store.wait()


def body(dims, dense_grads, dense_param, dense_acc, table, row_acc, touched, emb_grads):
    slows, fasts, ys, cores = dims
    shards = slows * fasts * ys * cores
    rows, wide = dense_param.shape
    f32 = jnp.float32
    count, width = emb_grads.shape
    grads = dense_grads.reshape(slows, fasts, ys, cores, rows, wide)
    racc = row_acc.reshape(-1, LANES)
    touched_rows = touched.reshape(-1, LANES)
    vmem = pl.BlockSpec(memory_space=pltpu.VMEM)
    hbm = pl.BlockSpec(memory_space=pl.ANY)
    quad = fasts * ys
    dma = pltpu.SemaphoreType.DMA
    block = jax.ShapeDtypeStruct((rows, wide), f32)
    per_row = jax.ShapeDtypeStruct((count, LANES), f32)
    own = (table, emb_grads, racc, dense_param, dense_acc)
    mean, clip, lane_hot, acc_at, held, emb, racc, param, acc = pl.pallas_call(
        functools.partial(exchange, dims),
        name="exchange",
        out_shape=(block, jax.ShapeDtypeStruct((1, LANES), f32), per_row, per_row)
        + tuple(jax.ShapeDtypeStruct(a.shape, f32) for a in own),
        in_specs=[pl.BlockSpec(memory_space=pltpu.HBM)] * 7,
        out_specs=(vmem,) * 9,
        scratch_shapes=[
            pltpu.VMEM((slows, fasts, ys, cores, rows, wide), f32),
            pltpu.VMEM((slows, fasts, ys, rows, wide), f32),
            pltpu.VMEM((slows, quad, rows, wide), f32),
            pltpu.VMEM((slows, quad, rows, wide), f32),
            pltpu.VMEM((slows, rows, wide), f32),
            pltpu.VMEM((slows, rows, wide), f32),
            pltpu.VMEM((shards, 1, LANES), f32),
            pltpu.SMEM((count,), jnp.int32),
            dma((slows,)),
            dma((slows,)),
            dma((slows,)),
            dma((slows, quad)),
            dma((slows, quad)),
            dma((slows,)),
            dma((slows,)),
            dma,
            dma,
            dma((6,)),
        ],
        compiler_params=pltpu.CompilerParams(
            collective_id=0, has_side_effects=True, vmem_limit_bytes=49 << 20
        ),
    )(*[pltpu.with_memory_space_constraint(a, pltpu.HBM) for a in (grads, emb_grads, racc, touched, table, dense_param, dense_acc)])
    _, new_table, new_dense, new_dense_acc, new_racc = pl.pallas_call(
        update,
        name="update",
        out_shape=(
            jax.ShapeDtypeStruct(table.shape, f32),
            jax.ShapeDtypeStruct(table.shape, f32),
            block,
            block,
            jax.ShapeDtypeStruct(racc.shape, f32),
        ),
        in_specs=[vmem, hbm] + [vmem] * 9,
        out_specs=(vmem,) + (hbm,) * 4,
        input_output_aliases={0: 0},
        scratch_shapes=[
            pltpu.VMEM((count, width), f32),
            pltpu.VMEM((count, LANES), f32),
            pltpu.VMEM((rows, wide), f32),
            pltpu.VMEM((rows, wide), f32),
            pltpu.VMEM(racc.shape, f32),
            pltpu.SMEM((count,), jnp.int32),
            dma((5,)),
        ],
        compiler_params=pltpu.CompilerParams(
            vmem_limit_bytes=2 * table.size * 4 + 8 * count * LANES * 4 + (4 << 20)
        ),
    )(held, touched, touched_rows, clip, mean, param, acc, emb, lane_hot, acc_at, racc)
    return new_dense, new_dense_acc, new_table, new_racc.reshape(-1)


def solution(mesh):
    wide, high = mesh.shape["gx"], mesh.shape["gy"]
    dims = (wide // 2, 2, high // 2, 2)
    return jax.shard_map(
        functools.partial(body, dims),
        mesh=mesh,
        in_specs=(
            P(("gx", "gy"), None, None),
            P(("gx", "gy"), None),
            P(("gx", "gy"), None),
            P(("gx", "gy"), None),
            P(("gx", "gy")),
            P(("gx", "gy")),
            P(("gx", "gy"), None),
        ),
        out_specs=(
            P(("gx", "gy"), None),
            P(("gx", "gy"), None),
            P(("gx", "gy"), None),
            P(("gx", "gy")),
        ),
        check_vma=False,
    )
```

```python
import functools

import jax
import jax.numpy as jnp
from jax import lax
from jax.experimental import pallas as pl
from jax.experimental.pallas import tpu as pltpu
from jax.sharding import PartitionSpec as P

learn_rate = 0.5
max_norm = 8.0
epsilon = 1e-10

MESH = pl.DeviceIdType.MESH
LANES = 128
UNROLL = 16


def flip(index, mask, size):
    result, bit = 0, 1
    while bit < size:
        digit = (index // bit) % 2
        result = result + bit * ((1 - digit) if mask & bit else digit)
        bit *= 2
    return result


def exchange(
    dims,
    grads,
    emb_hbm,
    racc_hbm,
    touched_hbm,
    table_hbm,
    param_hbm,
    dense_acc_hbm,
    mean_out,
    clip_out,
    lane_out,
    acc_out,
    table_out,
    emb,
    racc,
    param_out,
    dense_acc_out,
    own,
    pair_in,
    sums,
    plane_in,
    line_send,
    line_in,
    norms,
    touched,
    load_sem,
    pair_send_sem,
    pair_sem,
    plane_send_sem,
    plane_sem,
    line_send_sem,
    line_sem,
    norm_send_sem,
    norm_sem,
    side_sem,
):
    slows, fasts, ys, cores = dims
    gx, gy = lax.axis_index("gx"), lax.axis_index("gy")
    slow, fast = gx // fasts, gx % fasts
    y, core = gy // cores, gy % cores
    other = 1 - core
    plane = [(a, b) for a in reversed(range(fasts)) for b in reversed(range(ys)) if a or b]
    order = list(reversed(range(slows)))

    loads = {}
    for half, who in enumerate((other, core)):
        for k in order:
            loads[k, half] = pltpu.make_async_copy(
                grads.at[flip(slow, k, slows), :, :, who], own.at[k, :, :, who], load_sem.at[k, half]
            )
            loads[k, half].start()
    barrier = pltpu.get_barrier_semaphore()
    greet = [(gx, y * cores + other)]
    for a, b in plane:
        greet.append((slow * fasts + flip(fast, a, fasts), flip(y, b, ys) * cores + core))
    for k in range(1, slows):
        greet.append((flip(slow, k, slows) * fasts + fast, gy))
    for device in greet:
        pl.semaphore_signal(barrier, inc=1, device_id=device, device_id_type=MESH)
    pl.semaphore_wait(barrier, len(greet))

    pair = {}
    for k in order:
        loads[k, 0].wait()
        pair[k] = pltpu.make_async_remote_copy(
            src_ref=own.at[k, :, :, other],
            dst_ref=pair_in.at[k],
            send_sem=pair_send_sem.at[k],
            recv_sem=pair_sem.at[k],
            device_id=(gx, y * cores + other),
            device_id_type=MESH,
        )
        pair[k].start()

    sides = []
    held = (
        (emb_hbm, emb),
        (touched_hbm, touched),
        (racc_hbm, racc),
        (param_hbm, param_out),
        (dense_acc_hbm, dense_acc_out),
        (table_hbm, table_out),
    )
    for n, (source, target) in enumerate(held):
        sides.append(pltpu.make_async_copy(source, target, side_sem.at[n]))
        sides[-1].start()

    across = {}
    for k in order:
        loads[k, 1].wait()
        pair[k].wait_recv()
        for a in range(fasts):
            for b in range(ys):
                f, v = flip(fast, a, fasts), flip(y, b, ys)
                sums[k, a * ys + b] = own[k, f, v, core] + pair_in[k, f, v]
        for a, b in plane:
            q = a * ys + b
            across[k, q] = pltpu.make_async_remote_copy(
                src_ref=sums.at[k, q],
                dst_ref=plane_in.at[k, q],
                send_sem=plane_send_sem.at[k, q],
                recv_sem=plane_sem.at[k, q],
                device_id=(slow * fasts + flip(fast, a, fasts), flip(y, b, ys) * cores + core),
                device_id_type=MESH,
            )
            across[k, q].start()

    sides[0].wait()
    values = emb[...]
    emb_square = jnp.sum(values * values, axis=0, keepdims=True)

    def plane_total(k):
        total = sums[k, 0]
        for a, b in plane:
            across[k, a * ys + b].wait_recv()
            total = total + plane_in[k, a * ys + b]
        return total

    line = {}
    for k in order[:-1]:
        line_send[k] = plane_total(k)
        line[k] = pltpu.make_async_remote_copy(
            src_ref=line_send.at[k],
            dst_ref=line_in.at[k],
            send_sem=line_send_sem.at[k],
            recv_sem=line_sem.at[k],
            device_id=(flip(slow, k, slows) * fasts + fast, gy),
            device_id_type=MESH,
        )
        line[k].start()
    total = plane_total(0)
    for k in order[:-1]:
        line[k].wait_recv()
        total = total + line_in[k]

    shards = slows * fasts * ys * cores
    mean = total / jnp.float32(shards)
    mean_out[...] = mean
    square = mean * mean
    partial = square[:, :LANES]
    for start in range(LANES, square.shape[1], LANES):
        partial = partial + square[:, start : start + LANES]
    norms[0] = jnp.sum(partial, axis=0, keepdims=True) + emb_square

    width, height = slows * fasts, ys * cores
    spread = []
    for k in reversed(range(1, shards)):
        spread.append(
            pltpu.make_async_remote_copy(
                src_ref=norms.at[0],
                dst_ref=norms.at[k],
                send_sem=norm_send_sem,
                recv_sem=norm_sem,
                device_id=(flip(gx, k // height, width), flip(gy, k % height, height)),
                device_id_type=MESH,
            )
        )
        spread[-1].start()
    for side in sides[1:3]:
        side.wait()
    lane = lax.broadcasted_iota(jnp.int32, (1, LANES), 1)

    def gather(step, carry):
        for i in range(UNROLL):
            t = step * UNROLL + i
            row = touched[t]
            here = lane == row % LANES
            lane_out[pl.ds(t, 1), :] = jnp.where(here, 1.0, 0.0)
            acc_out[pl.ds(t, 1), :] = jnp.where(here, racc[pl.ds(row // LANES, 1), :], 0.0)
        return carry

    lax.fori_loop(0, touched.shape[0] // UNROLL, gather, 0)
    for start in range(0, touched.shape[0], LANES):
        part = pl.ds(start, LANES)
        found = jnp.sum(acc_out[part, :], axis=1, keepdims=True)
        acc_out[part, :] = jnp.broadcast_to(found, (LANES, LANES))

    everyone = pltpu.make_async_copy(
        norms.at[pl.ds(1, shards - 1)], norms.at[pl.ds(1, shards - 1)], norm_sem
    )
    everyone.wait()
    norm_sq = jnp.sum(jnp.sum(norms[...], axis=0), axis=1, keepdims=True)
    clip = jnp.minimum(jnp.float32(1.0), max_norm / (jnp.sqrt(norm_sq) + 1e-06))
    clip_out[...] = jnp.broadcast_to(clip, clip_out.shape)

    for side in sides[3:]:
        side.wait()
    for k in order:
        pair[k].wait_send()
    for copy in list(across.values()) + list(line.values()):
        copy.wait_send()
    pltpu.make_async_copy(
        norms.at[pl.ds(1, shards - 1)], norms.at[pl.ds(1, shards - 1)], norm_send_sem
    ).wait()


def update(
    table,
    touched_any,
    touched_rows,
    clip_ref,
    mean,
    dense_param,
    dense_acc,
    emb,
    lane_hot,
    acc_at,
    racc,
    held,
    new_table,
    new_dense,
    new_dense_acc,
    new_racc,
    change,
    placed,
    dense_v,
    acc_v,
    racc_v,
    touched,
    sems,
):
    numbers = pltpu.make_async_copy(touched_any, touched, sems.at[4])
    numbers.start()
    clip = clip_ref[:, :1]
    count, width = emb.shape

    def prepare(start):
        part = pl.ds(start, LANES)
        row_grads = clip * emb[part, :]
        square_mean = jnp.sum(row_grads * row_grads, axis=1, keepdims=True) / jnp.float32(width)
        updated_acc = acc_at[part, :] + square_mean
        change[part, :] = learn_rate * row_grads / (jnp.sqrt(updated_acc) + epsilon)
        placed[part, :] = lane_hot[part, :] * square_mean

    def scatter(start):
        for base in range(start, start + LANES, UNROLL):
            rows = [touched[base + i] for i in range(UNROLL)]
            fresh = [
                held[pl.ds(rows[i], 1), :] - change[pl.ds(base + i, 1), :] for i in range(UNROLL)
            ]
            for i in range(UNROLL):
                held[pl.ds(rows[i], 1), :] = fresh[i]

    starts = range(0, count, LANES)
    ahead = 2
    for start in starts[:ahead]:
        prepare(start)
    numbers.wait()
    for start in starts:
        if start + ahead * LANES < count:
            prepare(start + ahead * LANES)
        scatter(start)
    stores = [pltpu.make_async_copy(held, new_table, sems.at[0])]
    stores[0].start()

    def send(n, source, target):
        stores.append(pltpu.make_async_copy(source, target, sems.at[n]))
        stores[-1].start()

    scaled = clip * mean[...]
    acc = dense_acc[...] + scaled * scaled
    acc_v[...] = acc
    dense_v[...] = dense_param[...] - learn_rate * scaled / (jnp.sqrt(acc) + epsilon)
    send(1, acc_v, new_dense_acc)
    send(2, dense_v, new_dense)

    groups = lax.broadcasted_iota(jnp.int32, racc.shape, 0)
    added = racc[...]
    for start in starts:
        rows = touched_rows[start // LANES : start // LANES + 1, :]
        added = added + jnp.dot(
            jnp.where(groups == rows // LANES, 1.0, 0.0),
            placed[start : start + LANES, :],
            precision=lax.Precision.HIGHEST,
            preferred_element_type=jnp.float32,
        )
    racc_v[...] = added
    send(3, racc_v, new_racc)
    for store in stores:
        store.wait()


def body(dims, dense_grads, dense_param, dense_acc, table, row_acc, touched, emb_grads):
    slows, fasts, ys, cores = dims
    shards = slows * fasts * ys * cores
    rows, wide = dense_param.shape
    f32 = jnp.float32
    count, width = emb_grads.shape
    grads = dense_grads.reshape(slows, fasts, ys, cores, rows, wide)
    racc = row_acc.reshape(-1, LANES)
    touched_rows = touched.reshape(-1, LANES)
    vmem = pl.BlockSpec(memory_space=pltpu.VMEM)
    hbm = pl.BlockSpec(memory_space=pl.ANY)
    quad = fasts * ys
    dma = pltpu.SemaphoreType.DMA
    block = jax.ShapeDtypeStruct((rows, wide), f32)
    per_row = jax.ShapeDtypeStruct((count, LANES), f32)
    own = (table, emb_grads, racc, dense_param, dense_acc)
    mean, clip, lane_hot, acc_at, held, emb, racc, param, acc = pl.pallas_call(
        functools.partial(exchange, dims),
        name="exchange",
        out_shape=(block, jax.ShapeDtypeStruct((1, LANES), f32), per_row, per_row)
        + tuple(jax.ShapeDtypeStruct(a.shape, f32) for a in own),
        in_specs=[pl.BlockSpec(memory_space=pltpu.HBM)] * 7,
        out_specs=(vmem,) * 9,
        scratch_shapes=[
            pltpu.VMEM((slows, fasts, ys, cores, rows, wide), f32),
            pltpu.VMEM((slows, fasts, ys, rows, wide), f32),
            pltpu.VMEM((slows, quad, rows, wide), f32),
            pltpu.VMEM((slows, quad, rows, wide), f32),
            pltpu.VMEM((slows, rows, wide), f32),
            pltpu.VMEM((slows, rows, wide), f32),
            pltpu.VMEM((shards, 1, LANES), f32),
            pltpu.SMEM((count,), jnp.int32),
            dma((slows, 2)),
            dma((slows,)),
            dma((slows,)),
            dma((slows, quad)),
            dma((slows, quad)),
            dma((slows,)),
            dma((slows,)),
            dma,
            dma,
            dma((6,)),
        ],
        compiler_params=pltpu.CompilerParams(
            collective_id=0, has_side_effects=True, vmem_limit_bytes=49 << 20
        ),
    )(*[pltpu.with_memory_space_constraint(a, pltpu.HBM) for a in (grads, emb_grads, racc, touched, table, dense_param, dense_acc)])
    _, new_table, new_dense, new_dense_acc, new_racc = pl.pallas_call(
        update,
        name="update",
        out_shape=(
            jax.ShapeDtypeStruct(table.shape, f32),
            jax.ShapeDtypeStruct(table.shape, f32),
            block,
            block,
            jax.ShapeDtypeStruct(racc.shape, f32),
        ),
        in_specs=[vmem, hbm] + [vmem] * 9,
        out_specs=(vmem,) + (hbm,) * 4,
        input_output_aliases={0: 0},
        scratch_shapes=[
            pltpu.VMEM((count, width), f32),
            pltpu.VMEM((count, LANES), f32),
            pltpu.VMEM((rows, wide), f32),
            pltpu.VMEM((rows, wide), f32),
            pltpu.VMEM(racc.shape, f32),
            pltpu.SMEM((count,), jnp.int32),
            dma((5,)),
        ],
        compiler_params=pltpu.CompilerParams(
            vmem_limit_bytes=2 * table.size * 4 + 8 * count * LANES * 4 + (4 << 20)
        ),
    )(held, touched, touched_rows, clip, mean, param, acc, emb, lane_hot, acc_at, racc)
    return new_dense, new_dense_acc, new_table, new_racc.reshape(-1)


def solution(mesh):
    wide, high = mesh.shape["gx"], mesh.shape["gy"]
    dims = (wide // 2, 2, high // 2, 2)
    return jax.shard_map(
        functools.partial(body, dims),
        mesh=mesh,
        in_specs=(
            P(("gx", "gy"), None, None),
            P(("gx", "gy"), None),
            P(("gx", "gy"), None),
            P(("gx", "gy"), None),
            P(("gx", "gy")),
            P(("gx", "gy")),
            P(("gx", "gy"), None),
        ),
        out_specs=(
            P(("gx", "gy"), None),
            P(("gx", "gy"), None),
            P(("gx", "gy"), None),
            P(("gx", "gy")),
        ),
        check_vma=False,
    )
```
